32 devices in a mesh: rows: 16 (over z, y, x), cols: 2 (over core).
Axes of the slice: x: 2, y: 2, z: 4, core: 2. Of those that a mesh axis runs over, the one named last changes fastest.
Arguments:
- events: float32 [4096, 16384], P('rows', 'cols'), may hold values from -520 to 520
- sample_mask: int32 [4096, 128], P('rows', 'cols'), may hold values from 0 to 1, as said below
- keep_rate: float32 [128], P('cols'), may hold values from 0.25 to 1, as said below
Outputs:
- similarity: float32 [128, 16384], P('rows', 'cols')
The draws below stay inside these ranges and needn't reach their ends.
Inputs may be any that keep to these rules, and one draw needn't show every extreme that they name: `sample_mask`: each entry is 1 with probability keep_rate of its block, independently of all others. `keep_rate`: multiples of 1/1024.
All inputs are finite; a program needn't handle non-finite values.
Results may differ from the reference program's by a relative error of at most 0.0001.
Values sent between devices are 32-bit elements; how exact they have to be, the bound alone decides.
A program may use at most 64 MiB of HBM per device.

```python
import math
import jax
import jax.numpy as jnp
from jax import lax

COLUMNS = 16384
ROW_DEV = 256
QUERY_GROUP = 64
QUERIES = 128
MASK_BLOCKS = 128
ROWS = 4096
N_ROWS = 16
N_COLS = 2


def rate_levels(key):
    return jax.random.randint(jax.random.fold_in(key, 11), (MASK_BLOCKS,), 256, 1025)


def draw_keep_rate(key, part):
    return rate_levels(key).astype(jnp.float32) / 1024.0


def draw_sample_mask(key, part):
    levels = rate_levels(key)
    tickets = jax.random.randint(jax.random.fold_in(key, 12), (ROWS, MASK_BLOCKS), 0, 1024)
    return (tickets < levels[None, :]).astype(jnp.int32)


def draw_events(key, part):
    position = jnp.arange(ROWS, dtype=jnp.float32)
    rising = 1.0 + 2.0 * position / ROWS
    values = jnp.clip(jax.random.normal(jax.random.fold_in(key, 24), (ROWS, COLUMNS), jnp.float32), -6.0, 6.0)
    values = values * rising[:, None]
    return values.astype(jnp.float32)


def setup_inputs(seed: int = 0) -> dict:
    key_of = jax.random.split(jax.random.key(seed), 4)
    events = draw_events(jax.random.fold_in(key_of[3], 71), 0)
    sample_mask = draw_sample_mask(jax.random.fold_in(key_of[3], 71), 0)
    keep_rate = draw_keep_rate(jax.random.fold_in(key_of[3], 71), 0)
    return {"events": events, "sample_mask": sample_mask, "keep_rate": keep_rate}


def reference(events, sample_mask, keep_rate):
    span = COLUMNS // N_COLS
    order = jnp.arange(QUERIES, dtype=jnp.int32)
    source = (order // QUERY_GROUP * span + order % QUERY_GROUP).astype(jnp.int32)
    rates = jnp.repeat(keep_rate, 128)
    slabs = events.reshape(N_ROWS, ROW_DEV, COLUMNS)
    masks = sample_mask.reshape(N_ROWS, ROW_DEV, MASK_BLOCKS)

    def step(carry, inputs):
        gram, squares = carry
        slab, mask = inputs
        keep = jnp.repeat(mask, 128, axis=1).astype(slab.dtype)
        sampled = slab * keep
        picked = jnp.take(sampled, source, axis=1)
        gram = gram + lax.dot_general(picked, sampled, (((0,), (0,)), ((), ())), precision=lax.Precision.HIGHEST, preferred_element_type=gram.dtype)
        squares = squares + lax.optimization_barrier(jnp.sum(slab * slab, axis=0))
        return ((gram, squares), None)
    start = (jnp.zeros((QUERIES, COLUMNS), events.dtype), jnp.zeros((COLUMNS,), events.dtype))
    (gram, squares), _ = lax.scan(step, start, (slabs, masks))
    weight = lax.rsqrt(squares * rates + 1e-06)
    return math.sqrt(ROWS) * jnp.take(weight, source)[:, None] * gram * weight[None, :]
```

```python
import functools
import math

import jax
import jax.numpy as jnp
from jax import lax
from jax.experimental import pallas as pl
from jax.experimental.pallas import tpu as pltpu
from jax.sharding import PartitionSpec as P

QUERY_GROUP = 64
LANES = 128
SUBLANES = 8

epsilon = 1e-06

X, Y, LOW, HIGH, WIDE = 0, 1, 2, 3, 4
PLAN = (
    ((LOW, HIGH, Y, X), 1),
    ((X, LOW, Y, HIGH), 1),
    ((Y, LOW, X, HIGH), 1),
    ((Y, X, LOW, HIGH), 1),
    ((X, Y, WIDE), 1),
    ((Y, X, LOW, HIGH), 1),
    ((X, Y, LOW, HIGH), 2),
    ((LOW, X, HIGH, Y), 1),
    ((LOW, HIGH, X, Y), 1),
    ((Y, X, WIDE), 1),
    ((LOW, Y, X, HIGH), 1),
    ((Y, LOW, X, HIGH), 2),
    ((Y, X, LOW, HIGH), 2),
    ((LOW, Y, X, HIGH), 1),
    ((Y, X, LOW, HIGH), 2),
    ((Y, LOW, X, HIGH), 1),
    ((X, LOW, HIGH, Y), 1),
    ((Y, X, LOW, HIGH), 1),
    ((Y, X, LOW, HIGH), 1),
    ((X, Y, WIDE), 1),
    ((X, LOW, HIGH, Y), 2),
    ((LOW, X, Y, HIGH), 1),
    ((X, LOW, Y, HIGH), 1),
    ((X, Y, WIDE), 2),
    ((LOW, Y, X, HIGH), 1),
    ((LOW, X, Y, HIGH), 1),
)
SQUARES_PATH = (Y, X, LOW, HIGH)
GROUPS = (3, 5, 8, 8, 8)
HELD = (9, 10, 11, 12, 13, 14, 15, 16, 17, 18, 19, 20, 21, 22, 23, 24, 25, )
ORDERS = (
    (
        -27, 8, 16, 0, -10, -11, 32, 24, 56, -12, 40, -13, 208, 64, -14, 48, 72, -15,
        9, 25, -16, 1, -17, -18, 33, 17, 57, -19, 41, 209, -20, -21, 80, 73, -22, 88,
        65, 128, 104, 18, 58, 26, 42, 210, 152, 96, -23, 34, -24, -25, 49, 168, 74, 19,
        160, 27, 66, -26, 89, 43, 211, 112, 97, 129, 10, 176, 192, 120, 2, 50, 212, 136,
        130, 161, 184, 11, 144, 169, 81, 200, 90, 105, 59, 98, 51, 153, 113, 67, 3, 177,
        193, 137, 131, 145, 121, 162, 213, 82, 185, 201, 170, 91, 106, 178, 194, 114, 99, 138,
        122, 163, 214, 202, 154, 146, 83, 215, 171, 107, 186, 179, 195, 123, 115, 139, 147, 203,
    ),
    (
        -27, 0, 8, 16, -10, -11, 56, 32, 24, -12, 64, 40, -13, 208, 9, -14, 17, 48,
        72, -15, 57, -16, -17, -18, 33, 1, 25, 80, -19, 41, 209, -20, 18, -21, 73, -22,
        88, 104, 26, 65, 128, 42, 210, 152, 96, 34, 10, -23, -24, 58, 168, -25, 74, 49,
        160, 89, 66, 129, -26, 97, 112, 192, 176, 19, 27, 50, 43, 211, 120, 212, 161, 136,
        2, 11, 184, 81, 200, 169, 98, 90, 144, 177, 105, 113, 121, 153, 59, 130, 67, 213,
        137, 3, 193, 82, 201, 51, 185, 145, 170, 106, 178, 122, 114, 131, 214, 138, 194, 162,
        146, 91, 202, 99, 154, 215, 163, 186, 83, 171, 115, 107, 179, 139, 195, 147, 123, 203,
    ),
    (
        -27, 8, 16, -10, 0, -11, 32, 24, 56, -12, 40, -13, 208, -14, 64, 48, 1, 72,
        -15, 25, 9, -16, -17, -18, 33, 57, 17, -19, 41, 209, 65, -20, -21, 80, 73, -22,
        88, 128, 58, 104, 18, 26, 66, 34, 96, 42, 210, 152, 74, -23, -24, -25, 49, 2,
        168, 19, 160, 27, -26, 43, 211, 89, 129, 97, 112, 10, 176, 192, 120, 50, 136, 212,
        161, 184, 3, 144, 130, 169, 11, 81, 200, 59, 90, 105, 67, 98, 51, 153, 113, 177,
        162, 193, 137, 91, 121, 213, 99, 145, 82, 185, 131, 201, 170, 106, 178, 163, 194, 154,
        83, 122, 214, 114, 138, 146, 202, 171, 107, 179, 195, 115, 139, 123, 215, 203, 147, 186,
    ),
    (
        -27, 0, 8, 16, -10, -11, 32, 24, 56, 1, -12, 40, -13, 64, 208, -14, 48, 9,
        72, -15, 65, 25, -16, -17, 17, -18, 33, 57, 2, -19, 41, 209, -20, 58, -21, 80,
        73, -22, 66, 88, 104, 128, 18, 19, 26, 3, 34, 27, 42, 210, 74, 96, 152, 43,
        211, -23, -24, -25, 168, 49, 10, 11, 89, 160, -26, 129, 97, 130, 112, 192, 176, 50,
        120, 51, 212, 136, 161, 184, 144, 59, 169, 162, 200, 81, 67, 90, 98, 105, 177, 153,
        113, 131, 137, 193, 99, 145, 121, 91, 213, 154, 201, 185, 82, 83, 170, 114, 106, 163,
        178, 138, 194, 146, 122, 214, 202, 186, 171, 107, 179, 215, 123, 115, 139, 195, 147, 203,
    ),
)


def widen_blocks(values):
    spread = jnp.broadcast_to(values[..., None], values.shape + (128,))
    return spread.reshape(values.shape[:-1] + (values.shape[-1] * 128,))


def transposed_product(left, right):
    return lax.dot_general(
        left,
        right,
        (((0,), (0,)), ((), ())),
        precision=lax.Precision.HIGHEST,
        preferred_element_type=jnp.float32,
    )


def plain_shards(events, sample_mask, keep_rate):
    row_count, width = events.shape
    blocks = sample_mask.shape[1]
    keeping = sample_mask.astype(jnp.float32)[:, :, None]
    sampled = (events.reshape(row_count, blocks, 128) * keeping).reshape(row_count, width)
    local_squares = jnp.sum(events * events, axis=0)
    rates = widen_blocks(keep_rate)
    picked = sampled[:, :QUERY_GROUP]
    queries, query_part, query_rate = (
        lax.all_gather(picked, "cols", axis=1, tiled=True),
        lax.all_gather(local_squares[None, :QUERY_GROUP], "cols", axis=1, tiled=True),
        lax.all_gather(rates[None, :QUERY_GROUP], "cols", axis=1, tiled=True),
    )
    devices = lax.axis_size("rows")
    factor = math.sqrt(row_count * devices)
    count = queries.shape[1]
    share = count // devices
    place = lax.axis_index("rows")
    column_squares, query_squares = lax.psum((local_squares, query_part[0]), "rows")
    gram = lax.psum_scatter(
        transposed_product(queries, sampled), "rows", scatter_dimension=0, tiled=True
    )
    owned = lax.dynamic_slice_in_dim(query_squares * query_rate[0], place * share, share)
    query_weight = lax.rsqrt(owned + epsilon)
    column_weight = lax.rsqrt(column_squares * rates + epsilon)
    return factor * query_weight[:, None] * gram * column_weight[None, :]


def flipped(index, bit):
    step = 2**bit
    return index + step - 2 * step * ((index // step) % 2)


def split(values):
    high = values.astype(jnp.bfloat16)
    low = (values - high.astype(jnp.float32)).astype(jnp.bfloat16)
    return high, low


def steps_of(path, rows):
    left, found = rows, []
    for kind in path:
        if kind == WIDE:
            left //= 4
            sends = [(k * left, left, k << LOW) for k in (3, 2, 1)]
        else:
            left //= 2
            sends = [(left, left, 1 << kind)]
        found.append((left, sends))
    return found


def bits_of(path):
    return [b for kind in path for b in ((HIGH, LOW) if kind == WIDE else (kind,))]


def kernel(
    rows, cols, widths, groups,
    events_ref, mask_ref, rate_ref,
    gram_out, weight_out,
    events, gram, inbox, first, queries, squares, squares_inbox, totals, query_weight,
    mask_in, rate_in, mask, load_sem, first_sem, far_sem, query_send, query_recv, weight_send, weight_recv,
    send_sem, recv_sem, squares_send, squares_recv,
):
    bits = rows.bit_length() - 1
    quad = rows // 4
    me, mine = lax.axis_index("rows"), lax.axis_index("cols")
    level = me // quad
    row_count, width = events.shape
    blocks = mask_ref.shape[0]
    share = gram.shape[1]
    count = rows * share
    starts = [sum(widths[:c]) for c in range(len(widths))]
    last = len(widths)

    heads = [
        pltpu.make_async_copy(mask_ref, mask_in, first_sem.at[0]),
        pltpu.make_async_copy(events_ref.at[:, pl.ds(0, LANES)], first, first_sem.at[1]),
        pltpu.make_async_copy(rate_ref, rate_in, first_sem.at[2]),
    ]
    for head in heads:
        head.start()
    loads = []
    for g, (start, size) in enumerate(groups):
        place = pl.ds(start, size)
        load = pltpu.make_async_copy(events_ref.at[:, place], events.at[:, place], load_sem.at[g])
        loads.append(load)
    for load in loads[:2]:
        load.start()

    partners = {1 << b: flipped(me, b) for b in range(bits)}
    partners[1 << LOW | 1 << HIGH] = flipped(partners[1 << LOW], HIGH)
    peers = [lax.rem(mine + j, cols) for j in range(1, cols)]
    barrier = pltpu.get_barrier_semaphore()
    for b in (X, Y):
        pl.semaphore_signal(barrier, inc=1, device_id={"rows": partners[1 << b]})
    for peer in peers:
        pl.semaphore_signal(barrier, inc=1, device_id={"cols": peer})

    @pl.when(level > 0)
    def _():
        pl.semaphore_signal(barrier, inc=1, device_id={"rows": me - quad})

    @pl.when(level < 3)
    def _():
        pl.semaphore_signal(barrier, inc=1, device_id={"rows": me + quad})

    for head in heads[:2]:
        head.wait()
    keeping = mask_in[...].astype(jnp.float32)
    queries[mine] = first[...].T[:QUERY_GROUP] * keeping[0:1]
    pl.semaphore_wait(barrier, cols + 2 + (level * (3 - level) + 1) // 2)

    shared = []
    for j, peer in enumerate(peers):
        copy = pltpu.make_async_remote_copy(
            src_ref=queries.at[mine], dst_ref=queries.at[mine],
            send_sem=query_send.at[j], recv_sem=query_recv.at[j], device_id={"cols": peer},
        )
        copy.start()
        shared.append(copy)

    for load in loads[2:]:
        load.start()

    @pl.when((level == 1) | (level == 2))
    def _():
        pl.semaphore_signal(far_sem.at[0], inc=1, device_id={"rows": me - quad})
        pl.semaphore_signal(far_sem.at[0], inc=1, device_id={"rows": me + quad})

    mask[...] = keeping.T.astype(jnp.bfloat16)
    for copy in shared:
        copy.wait()
    high, low = split(jnp.concatenate([queries[j] for j in range(cols)], axis=0))
    both = jnp.concatenate([high, low], axis=0)

    own = [(me // 2**b) % 2 for b in range(bits)]
    kept_slots = {}

    def slots(path):
        order = bits_of(path)
        if tuple(order) not in kept_slots:
            parts = []
            for k, b in enumerate(order):
                weight = 2 ** (bits - 1 - k)
                same = own[b] * weight
                parts.append((same, weight - same))
            half = bits // 2
            upper, lower = {}, {}
            for pick in range(2**half):
                upper[pick] = sum(parts[k][pick >> k & 1] for k in range(half))
                lower[pick] = sum(parts[half + k][pick >> k & 1] for k in range(half))
            found = []
            for d in range(rows):
                picks = [d >> b & 1 for b in order]
                found.append(
                    upper[sum(p << k for k, p in enumerate(picks[:half]))]
                    + lower[sum(p << k for k, p in enumerate(picks[half:]))]
                )
            kept_slots[tuple(order)] = found
        return kept_slots[tuple(order)]

    walks = [steps_of(path, rows) for path, _ in PLAN]
    marks = {}
    for c, walk in enumerate(walks):
        for s in range(len(walk)):
            marks[c, s] = len(marks)

    def exchange(c, s, k):
        slot, size, flips = walks[c][s][1][k]
        part = (pl.ds(slot, size), slice(None), pl.ds(starts[c], widths[c]))
        return pltpu.make_async_remote_copy(
            src_ref=gram.at[part], dst_ref=inbox.at[part],
            send_sem=send_sem, recv_sem=recv_sem.at[marks[c, s]], device_id={"rows": partners[flips]},
        )

    def exchanges(c, s):
        return [exchange(c, s, k) for k in range(len(walks[c][s][1]))]

    def square_range(s, sent):
        at = 0
        for k in range(s + 1):
            bit = own[SQUARES_PATH[k]]
            if k == s and sent:
                bit = 1 - bit
            at = at + bit * (width // 2 ** (k + 1))
        return pl.ds(pl.multiple_of(at, LANES), width // 2 ** (s + 1))

    def square_exchange(s):
        if s < bits:
            place = square_range(s, True)
            source, target, b = squares.at[:, place], squares_inbox.at[s, :, place], SQUARES_PATH[s]
        else:
            b = 2 * bits - 1 - s
            place = square_range(b, False)
            source, target, b = totals.at[:, place], totals.at[:, place], SQUARES_PATH[b]
        return pltpu.make_async_remote_copy(
            src_ref=source, dst_ref=target,
            send_sem=squares_send, recv_sem=squares_recv.at[s], device_id={"rows": partners[1 << b]},
        )

    def weight_exchange(j):
        return pltpu.make_async_remote_copy(
            src_ref=query_weight.at[mine], dst_ref=query_weight.at[mine],
            send_sem=weight_send.at[j], recv_sem=weight_recv.at[j], device_id={"cols": peers[j]},
        )

    for g, (start, size) in enumerate(groups):
        loads[g].wait()
        place = pl.ds(start, size)
        values = events[:, place]
        squares[:, place] = jnp.sum(values * values, axis=0, keepdims=True)
        block_of = lax.broadcasted_iota(jnp.int32, (blocks, size), 1) // LANES + start // LANES
        spread = lax.broadcasted_iota(jnp.int32, (blocks, size), 0) == block_of
        spread = spread.astype(jnp.float32).astype(jnp.bfloat16)
        kept = values * jnp.dot(mask[...], spread, preferred_element_type=jnp.float32)
        kept_high, kept_low = split(kept)
        pair = jnp.dot(both, kept_high, preferred_element_type=jnp.float32)
        rest = jnp.dot(high, kept_low, preferred_element_type=jnp.float32)
        product = pair[:count] + (pair[count:] + rest)
        for c in range(last):
            begin, end = max(start, starts[c]), min(start + size, starts[c] + widths[c])
            if begin < end:
                chosen = slots(PLAN[c][0])
                for d in range(rows):
                    gram[chosen[d], :, pl.ds(begin, end - begin)] = product[d * share : (d + 1) * share, begin - start : end - start]
            if begin < end == starts[c] + widths[c] and c not in HELD:
                for copy in exchanges(c, 0):
                    copy.start()

    heads[2].wait()
    pl.semaphore_wait(far_sem.at[0], 1)
    pl.semaphore_signal(far_sem.at[1], inc=1, device_id={"rows": partners[1 << LOW]})
    pl.semaphore_wait(far_sem.at[1], 1)

    def issue(c):
        if c == last:
            square_exchange(0).start()
        else:
            for copy in exchanges(c, 0):
                copy.start()

    def add_squares(s):
        square_exchange(s).wait_recv()
        if s < bits:
            place = square_range(s, False)
            value = squares[:, place] + squares_inbox[s, :, place]
            if s < bits - 1:
                squares[:, place] = value
            else:
                totals[:, place] = value
        if s < 2 * bits - 1:
            square_exchange(s + 1).start()
            return
        query_weight[mine] = jnp.broadcast_to(
            lax.rsqrt(totals[:, pl.ds(0, LANES)] * rate_in[0, 0] + epsilon), (SUBLANES, LANES)
        )
        for j in range(len(peers)):
            weight_exchange(j).start()

        def widen(b, carry):
            place = pl.ds(pl.multiple_of(b * LANES, LANES), LANES)
            weight_out[:, place] = lax.rsqrt(totals[:, place] * rate_in[0, b] + epsilon)
            return carry

        lax.fori_loop(0, blocks, widen, 0)

    def add(c, s):
        if c == last:
            add_squares(s)
            return
        left, sends = walks[c][s]
        place = pl.ds(starts[c], widths[c])
        arrived = (pl.ds(left, sum(size for _, size, _ in sends)), slice(None), place)
        pltpu.make_async_remote_copy(
            src_ref=gram.at[arrived], dst_ref=inbox.at[arrived],
            send_sem=send_sem, recv_sem=recv_sem.at[marks[c, s]], device_id={"rows": partners[1]},
        ).wait_recv()
        total = gram[pl.ds(0, left), :, place]
        for slot, size, _ in reversed(sends):
            total = total + inbox[pl.ds(slot, size), :, place]
        if s < len(walks[c]) - 1:
            gram[pl.ds(0, left), :, place] = total
            for copy in exchanges(c, s + 1):
                copy.start()
        else:
            gram_out[:, place] = total[0]

    def run(order):
        for code in order:
            if code < 0:
                issue(-1 - code)
            else:
                add(code // 8, code % 8)

    for z, order in enumerate(ORDERS):
        pl.when(level == z)(functools.partial(run, order))

    for j in range(len(peers)):
        weight_exchange(j).wait()
    factor = math.sqrt(row_count * rows)
    weights = jnp.concatenate([query_weight[j, 0:1, :QUERY_GROUP] for j in range(cols)], axis=1)
    owner = lax.broadcasted_iota(jnp.int32, (share, count), 0) + me * share
    lane = lax.broadcasted_iota(jnp.int32, (share, count), 1)
    weight = jnp.sum(jnp.where(owner == lane, factor * weights, 0.0), axis=1, keepdims=True)
    gram_out[...] = gram_out[...] * weight
    rest = pl.ds(1, rows - 1)
    pltpu.make_async_remote_copy(
        src_ref=gram.at[rest], dst_ref=inbox.at[rest],
        send_sem=send_sem, recv_sem=recv_sem.at[0], device_id={"rows": partners[1]},
    ).wait_send()
    rest = (pl.ds(0, 2), slice(None), pl.ds(0, width // rows * (rows - 1)))
    pltpu.make_async_remote_copy(
        src_ref=squares_inbox.at[rest], dst_ref=squares_inbox.at[rest],
        send_sem=squares_send, recv_sem=squares_recv.at[0], device_id={"rows": partners[1]},
    ).wait_send()


def kernel_shards(rows, cols, widths, groups, events, sample_mask, keep_rate):
    row_count, width = events.shape
    blocks = sample_mask.shape[1]
    bits = rows.bit_length() - 1
    count = QUERY_GROUP * cols
    share = count // rows
    steps = sum(len(path) for path, _ in PLAN)
    vmem = pl.BlockSpec(memory_space=pltpu.VMEM)
    dma = pltpu.SemaphoreType.DMA
    gram, weight = pl.pallas_call(
        functools.partial(kernel, rows, cols, widths, groups),
        out_shape=(
            jax.ShapeDtypeStruct((share, width), jnp.float32),
            jax.ShapeDtypeStruct((1, width), jnp.float32),
        ),
        in_specs=[pl.BlockSpec(memory_space=pl.ANY)] * 3,
        out_specs=(vmem, vmem),
        scratch_shapes=[
            pltpu.VMEM((row_count, width), jnp.float32),
            pltpu.VMEM((rows, share, width), jnp.float32),
            pltpu.VMEM((rows, share, width), jnp.float32),
            pltpu.VMEM((row_count, LANES), jnp.float32),
            pltpu.VMEM((cols, QUERY_GROUP, row_count), jnp.float32),
            pltpu.VMEM((1, width), jnp.float32),
            pltpu.VMEM((bits, 1, width), jnp.float32),
            pltpu.VMEM((1, width), jnp.float32),
            pltpu.VMEM((cols, SUBLANES, LANES), jnp.float32),
            pltpu.VMEM((blocks, row_count), jnp.int32),
            pltpu.SMEM((1, blocks), jnp.float32),
            pltpu.VMEM((row_count, blocks), jnp.bfloat16),
            dma((len(groups),)),
            dma((3,)),
            pltpu.SemaphoreType.REGULAR((2,)),
            dma((cols - 1,)),
            dma((cols - 1,)),
            dma((cols - 1,)),
            dma((cols - 1,)),
            dma,
            dma((steps,)),
            dma,
            dma((2 * bits,)),
        ],
        compiler_params=pltpu.CompilerParams(
            collective_id=0, has_side_effects=True, vmem_limit_bytes=48 * 2**20
        ),
    )(
        events,
        pltpu.with_memory_space_constraint(sample_mask.T, pltpu.HBM),
        pltpu.with_memory_space_constraint(keep_rate[None, :], pltpu.HBM),
    )
    return gram * weight


def solution(mesh):
    placed = (P("rows", "cols"), P("rows", "cols"), P("cols"))
    rows, cols = mesh.shape["rows"], mesh.shape["cols"]
    count = QUERY_GROUP * cols
    units = sum(size for _, size in PLAN)

    def shards(events, sample_mask, keep_rate):
        width = events.shape[1]
        fits = rows == 2 ** len(SQUARES_PATH) and count == rows * SUBLANES and width % (units * LANES) == 0 and cols > 1
        if not fits:
            return plain_shards(events, sample_mask, keep_rate)
        widths = [width // units * size for _, size in PLAN]
        sizes = [width // units * size for size in GROUPS]
        groups = [(sum(sizes[:g]), size) for g, size in enumerate(sizes)]
        return kernel_shards(rows, cols, widths, groups, events, sample_mask, keep_rate)

    return jax.shard_map(
        shards, mesh=mesh, in_specs=placed, out_specs=P("rows", "cols"), check_vma=False
    )
```

```python
import functools
import math

import jax
import jax.numpy as jnp
from jax import lax
from jax.experimental import pallas as pl
from jax.experimental.pallas import tpu as pltpu
from jax.sharding import PartitionSpec as P

QUERY_GROUP = 64
LANES = 128
SUBLANES = 8

epsilon = 1e-06

X, Y, LOW, HIGH, WIDE = 0, 1, 2, 3, 4
PLAN = (
    ((X, WIDE, Y), 4),
    ((Y, WIDE, X), 4),
    ((LOW, HIGH, X, Y), 4),
    ((LOW, Y, X, HIGH), 2),
    ((X, Y, LOW, HIGH), 4),
    ((LOW, Y, X, HIGH), 2),
    ((LOW, Y, X, HIGH), 2),
    ((Y, X, LOW, HIGH), 4),
    ((Y, X, WIDE), 4),
    ((LOW, Y, X, HIGH), 2),
    ((X, LOW, HIGH, Y), 2),
    ((X, Y, WIDE), 2),
    ((X, Y, WIDE), 2),
    ((Y, WIDE, X), 2),
    ((Y, X, WIDE), 2),
    ((X, Y, WIDE), 2),
    ((Y, X, LOW, HIGH), 2),
    ((X, Y, WIDE), 2),
    ((Y, X, WIDE), 2),
    ((X, Y, LOW, HIGH), 2),
    ((X, LOW, Y, HIGH), 4),
    ((Y, X, WIDE), 2),
    ((X, Y, WIDE), 2),
    ((LOW, Y, X, HIGH), 2),
    ((LOW, Y, X, HIGH), 2),
)
SQUARES_PATH = (X, Y, LOW, HIGH)
GROUPS = (12, 20, 16, 16)
EARLY = 3
HELD = (10, 11, 12, 13, 14, 15, 16, 17, 18, 19, 20, 21, 22, 23, 24, )
ORDERS = (
    (
        -26, -11, 0, 8, 16, -12, 24, -13, 32, 56, 200, -14, 40, -15, -16, 80, -17, -18,
        48, -19, 64, -20, -21, 88, 25, 96, -22, 33, 201, 17, -23, 57, 72, 104, -24, 41,
        120, 1, 112, 136, 81, 9, 128, 65, 34, 202, 49, -25, 58, 152, 144, 89, 184, 97,
        105, 82, 160, 26, 168, 35, 203, 18, 73, 121, 2, 192, 176, 66, 42, 137, 113, 59,
        153, 10, 204, 27, 185, 129, 83, 50, 19, 161, 90, 205, 145, 193, 106, 43, 177, 169,
        74, 154, 98, 186, 122, 162, 130, 206, 194, 138, 51, 114, 75, 146, 207, 187, 178, 163,
        170, 131, 155, 195,
    ),
    (
        -26, -11, 16, 0, 8, 24, -12, 40, -13, 32, 56, 200, -14, -15, 48, -16, 80, -17,
        -18, 72, -19, 64, -20, -21, 88, 25, 41, 96, -22, 33, 201, -23, 57, 17, -24, 104,
        120, 1, 112, 81, 136, 49, 34, 202, 9, 65, 58, 128, -25, 73, 152, 105, 184, 144,
        89, 97, 160, 26, 42, 82, 168, 35, 203, 192, 121, 66, 176, 2, 204, 18, 137, 113,
        153, 50, 10, 59, 161, 185, 83, 90, 129, 74, 193, 106, 177, 145, 19, 98, 154, 205,
        169, 27, 130, 186, 162, 122, 194, 138, 114, 206, 43, 146, 178, 207, 170, 51, 75, 155,
        187, 131, 163, 195,
    ),
    (
        -26, -11, 0, 8, 16, -12, 24, -13, 32, 56, 200, -14, 40, -15, -16, 80, -17, 48,
        -18, -19, 64, -20, -21, 88, 72, 25, 96, -22, 33, 201, -23, 57, 104, -24, 1, 41,
        120, 17, 112, 136, 9, 81, 128, 65, 34, 49, 202, -25, 152, 105, 144, 82, 89, 184,
        73, 58, 35, 97, 203, 160, 26, 168, 66, 2, 59, 176, 42, 121, 192, 18, 137, 113,
        90, 153, 10, 83, 27, 204, 129, 185, 50, 43, 161, 106, 177, 98, 145, 193, 74, 19,
        122, 205, 169, 51, 138, 186, 114, 162, 130, 154, 194, 206, 75, 146, 155, 187, 163, 178,
        131, 195, 170, 207,
    ),
    (
        -26, -11, 16, 0, 8, -12, 24, 17, -13, 32, 56, 200, -14, -15, -16, 80, -17, 40,
        -18, -19, 64, -20, -21, 88, 25, 18, -22, 33, 48, 201, 96, -23, 72, 104, -24, 57,
        1, 9, 112, 120, 81, 128, 136, 41, 34, 202, 82, 65, 35, 203, -25, 144, 58, 89,
        105, 152, 19, 168, 59, 184, 49, 66, 160, 97, 26, 73, 2, 176, 27, 121, 192, 10,
        204, 90, 98, 137, 113, 83, 129, 153, 42, 43, 185, 145, 106, 177, 161, 122, 138, 169,
        193, 114, 50, 51, 74, 154, 75, 205, 186, 130, 178, 162, 194, 206, 146, 155, 170, 131,
        187, 163, 195, 207,
    ),
)


def widen_blocks(values):
    spread = jnp.broadcast_to(values[..., None], values.shape + (128,))
    return spread.reshape(values.shape[:-1] + (values.shape[-1] * 128,))


def transposed_product(left, right):
    return lax.dot_general(
        left,
        right,
        (((0,), (0,)), ((), ())),
        precision=lax.Precision.HIGHEST,
        preferred_element_type=jnp.float32,
    )


def plain_shards(events, sample_mask, keep_rate):
    row_count, width = events.shape
    blocks = sample_mask.shape[1]
    keeping = sample_mask.astype(jnp.float32)[:, :, None]
    sampled = (events.reshape(row_count, blocks, 128) * keeping).reshape(row_count, width)
    local_squares = jnp.sum(events * events, axis=0)
    rates = widen_blocks(keep_rate)
    picked = sampled[:, :QUERY_GROUP]
    queries, query_part, query_rate = (
        lax.all_gather(picked, "cols", axis=1, tiled=True),
        lax.all_gather(local_squares[None, :QUERY_GROUP], "cols", axis=1, tiled=True),
        lax.all_gather(rates[None, :QUERY_GROUP], "cols", axis=1, tiled=True),
    )
    devices = lax.axis_size("rows")
    factor = math.sqrt(row_count * devices)
    count = queries.shape[1]
    share = count // devices
    place = lax.axis_index("rows")
    column_squares, query_squares = lax.psum((local_squares, query_part[0]), "rows")
    gram = lax.psum_scatter(
        transposed_product(queries, sampled), "rows", scatter_dimension=0, tiled=True
    )
    owned = lax.dynamic_slice_in_dim(query_squares * query_rate[0], place * share, share)
    query_weight = lax.rsqrt(owned + epsilon)
    column_weight = lax.rsqrt(column_squares * rates + epsilon)
    return factor * query_weight[:, None] * gram * column_weight[None, :]


def flipped(index, bit):
    step = 2**bit
    return index + step - 2 * step * ((index // step) % 2)


def split(values):
    high = values.astype(jnp.bfloat16)
    low = (values - high.astype(jnp.float32)).astype(jnp.bfloat16)
    return high, low


def steps_of(path, rows):
    left, found = rows, []
    for kind in path:
        if kind == WIDE:
            left //= 4
            sends = [(k * left, left, k << LOW) for k in (3, 2, 1)]
        else:
            left //= 2
            sends = [(left, left, 1 << kind)]
        found.append((left, sends))
    return found


def bits_of(path):
    return [b for kind in path for b in ((HIGH, LOW) if kind == WIDE else (kind,))]


def kernel(
    rows, cols, widths, groups,
    events_ref, mask_ref, rate_ref,
    gram_out, weight_out,
    events, gram, inbox, first, queries, squares, squares_inbox, totals, query_weight,
    mask_in, rate_in, mask, load_sem, first_sem, far_sem, query_send, query_recv, weight_send, weight_recv,
    send_sem, recv_sem, squares_send, squares_recv,
):
    bits = rows.bit_length() - 1
    quad = rows // 4
    me, mine = lax.axis_index("rows"), lax.axis_index("cols")
    level = me // quad
    row_count, width = events.shape
    blocks = mask_ref.shape[0]
    share = gram.shape[1]
    count = rows * share
    starts = [sum(widths[:c]) for c in range(len(widths))]
    last = len(widths)

    heads = [
        pltpu.make_async_copy(mask_ref, mask_in, first_sem.at[0]),
        pltpu.make_async_copy(events_ref.at[:, pl.ds(0, LANES)], first, first_sem.at[1]),
        pltpu.make_async_copy(rate_ref, rate_in, first_sem.at[2]),
    ]
    for head in heads:
        head.start()
    loads = []
    for g, (start, size) in enumerate(groups):
        place = pl.ds(start, size)
        load = pltpu.make_async_copy(events_ref.at[:, place], events.at[:, place], load_sem.at[g])
        loads.append(load)
    for load in loads[:1]:
        load.start()

    partners = {1 << b: flipped(me, b) for b in range(bits)}
    partners[1 << LOW | 1 << HIGH] = flipped(partners[1 << LOW], HIGH)
    peers = [lax.rem(mine + j, cols) for j in range(1, cols)]
    barrier = pltpu.get_barrier_semaphore()
    for b in (X, Y):
        pl.semaphore_signal(barrier, inc=1, device_id={"rows": partners[1 << b]})
    for peer in peers:
        pl.semaphore_signal(barrier, inc=1, device_id={"cols": peer})

    @pl.when(level > 0)
    def _():
        pl.semaphore_signal(barrier, inc=1, device_id={"rows": me - quad})

    @pl.when(level < 3)
    def _():
        pl.semaphore_signal(barrier, inc=1, device_id={"rows": me + quad})

    for head in heads[:2]:
        head.wait()
    keeping = mask_in[...].astype(jnp.float32)
    queries[mine] = first[...].T[:QUERY_GROUP] * keeping[0:1]
    pl.semaphore_wait(barrier, cols + 2 + (level * (3 - level) + 1) // 2)

    shared = []
    for j, peer in enumerate(peers):
        copy = pltpu.make_async_remote_copy(
            src_ref=queries.at[mine], dst_ref=queries.at[mine],
            send_sem=query_send.at[j], recv_sem=query_recv.at[j], device_id={"cols": peer},
        )
        copy.start()
        shared.append(copy)

    for load in loads[1:]:
        load.start()

    @pl.when((level == 1) | (level == 2))
    def _():
        pl.semaphore_signal(far_sem.at[0], inc=1, device_id={"rows": me - quad})
        pl.semaphore_signal(far_sem.at[0], inc=1, device_id={"rows": me + quad})

    mask[...] = keeping.T.astype(jnp.bfloat16)

    own = [(me // 2**b) % 2 for b in range(bits)]
    kept_slots = {}

    def slots(path, other=None):
        order = bits_of(path)
        key = tuple(order), other is None
        if other is None and key in kept_slots:
            return kept_slots[key]
        parts = []
        for k, b in enumerate(order):
            weight = 2 ** (bits - 1 - k)
            same = own[b] * weight
            parts.append((same, weight - same) if other is None or b != HIGH else (other * weight, 0))
        half = bits // 2
        upper, lower = {}, {}
        for pick in range(2**half):
            upper[pick] = sum(parts[k][pick >> k & 1] for k in range(half))
            lower[pick] = sum(parts[half + k][pick >> k & 1] for k in range(half))
        found = []
        for d in range(rows if other is None else rows // 2):
            picks = [d >> b & 1 for b in order]
            found.append(
                upper[sum(p << k for k, p in enumerate(picks[:half]))]
                + lower[sum(p << k for k, p in enumerate(picks[half:]))]
            )
        if other is None:
            kept_slots[key] = found
        return found

    walks = [steps_of(path, rows) for path, _ in PLAN]
    marks = {}
    for c, walk in enumerate(walks):
        for s in range(len(walk)):
            marks[c, s] = len(marks)

    def exchange(c, s, k):
        slot, size, flips = walks[c][s][1][k]
        part = (pl.ds(slot, size), slice(None), pl.ds(starts[c], widths[c]))
        return pltpu.make_async_remote_copy(
            src_ref=gram.at[part], dst_ref=inbox.at[part],
            send_sem=send_sem, recv_sem=recv_sem.at[marks[c, s]], device_id={"rows": partners[flips]},
        )

    def exchanges(c, s):
        return [exchange(c, s, k) for k in range(len(walks[c][s][1]))]

    def square_range(s, sent):
        at = 0
        for k in range(s + 1):
            bit = own[SQUARES_PATH[k]]
            if k == s and sent:
                bit = 1 - bit
            at = at + bit * (width // 2 ** (k + 1))
        return pl.ds(pl.multiple_of(at, LANES), width // 2 ** (s + 1))

    def square_exchange(s):
        if s < bits:
            place = square_range(s, True)
            source, target, b = squares.at[:, place], squares_inbox.at[s, :, place], SQUARES_PATH[s]
        else:
            b = 2 * bits - 1 - s
            place = square_range(b, False)
            source, target, b = totals.at[:, place], totals.at[:, place], SQUARES_PATH[b]
        return pltpu.make_async_remote_copy(
            src_ref=source, dst_ref=target,
            send_sem=squares_send, recv_sem=squares_recv.at[s], device_id={"rows": partners[1 << b]},
        )

    def weight_exchange(j):
        return pltpu.make_async_remote_copy(
            src_ref=query_weight.at[mine], dst_ref=query_weight.at[mine],
            send_sem=weight_send.at[j], recv_sem=weight_recv.at[j], device_id={"cols": peers[j]},
        )

    def sampled(g):
        start, size = groups[g]
        loads[g].wait()
        place = pl.ds(start, size)
        values = events[:, place]
        squares[:, place] = jnp.sum(values * values, axis=0, keepdims=True)
        block_of = lax.broadcasted_iota(jnp.int32, (blocks, size), 1) // LANES + start // LANES
        spread = lax.broadcasted_iota(jnp.int32, (blocks, size), 0) == block_of
        spread = spread.astype(jnp.float32).astype(jnp.bfloat16)
        return split(values * jnp.dot(mask[...], spread, preferred_element_type=jnp.float32))

    def multiplied(rows_split, kept):
        high, low = rows_split
        lines = high.shape[0]
        both = jnp.concatenate([high, low], axis=0)
        pair = jnp.dot(both, kept[0], preferred_element_type=jnp.float32)
        rest = jnp.dot(high, kept[1], preferred_element_type=jnp.float32)
        return pair[:lines] + (pair[lines:] + rest)

    def half_send(c, whose):
        slot, size, flips = walks[c][0][1][0]
        part = size // 2
        at = slot + (whose + own[HIGH] - 2 * whose * own[HIGH]) * part
        place = (pl.ds(at, part), slice(None), pl.ds(starts[c], widths[c]))
        return pltpu.make_async_remote_copy(
            src_ref=gram.at[place], dst_ref=inbox.at[place],
            send_sem=send_sem, recv_sem=recv_sem.at[marks[c, 0]], device_id={"rows": partners[flips]},
        )

    start, size = groups[0]
    kept = sampled(0)
    for turn in range(cols):
        whose = lax.rem(mine + turn, cols)
        if turn:
            for copy in shared:
                copy.wait()
        product = multiplied(split(queries[whose]), kept)
        for c in range(EARLY):
            other = whose + own[HIGH] - 2 * whose * own[HIGH]
            chosen = slots(PLAN[c][0], other)
            for d in range(rows // cols):
                gram[chosen[d], :, pl.ds(starts[c], widths[c])] = product[
                    d * share : (d + 1) * share, starts[c] : starts[c] + widths[c]
                ]
            half_send(c, whose).start()

    everyone = split(jnp.concatenate([queries[j] for j in range(cols)], axis=0))
    for g in range(1, len(groups)):
        start, size = groups[g]
        product = multiplied(everyone, sampled(g))
        for c in range(EARLY, last):
            begin, end = max(start, starts[c]), min(start + size, starts[c] + widths[c])
            if begin < end:
                chosen = slots(PLAN[c][0])
                for d in range(rows):
                    gram[chosen[d], :, pl.ds(begin, end - begin)] = product[d * share : (d + 1) * share, begin - start : end - start]
            if begin < end == starts[c] + widths[c] and c not in HELD:
                for copy in exchanges(c, 0):
                    copy.start()

    heads[2].wait()
    pl.semaphore_wait(far_sem.at[0], 1)
    pl.semaphore_signal(far_sem.at[1], inc=1, device_id={"rows": partners[1 << LOW]})
    pl.semaphore_wait(far_sem.at[1], 1)

    def issue(c):
        if c == last:
            square_exchange(0).start()
        else:
            for copy in exchanges(c, 0):
                copy.start()

    def add_squares(s):
        square_exchange(s).wait_recv()
        if s < bits:
            place = square_range(s, False)
            value = squares[:, place] + squares_inbox[s, :, place]
            if s < bits - 1:
                squares[:, place] = value
            else:
                totals[:, place] = value
        if s < 2 * bits - 1:
            square_exchange(s + 1).start()
            return
        query_weight[mine] = jnp.broadcast_to(
            lax.rsqrt(totals[:, pl.ds(0, LANES)] * rate_in[0, 0] + epsilon), (SUBLANES, LANES)
        )
        for j in range(len(peers)):
            weight_exchange(j).start()

        def widen(b, carry):
            place = pl.ds(pl.multiple_of(b * LANES, LANES), LANES)
            weight_out[:, place] = lax.rsqrt(totals[:, place] * rate_in[0, b] + epsilon)
            return carry

        lax.fori_loop(0, blocks, widen, 0)

    def add(c, s):
        if c == last:
            add_squares(s)
            return
        left, sends = walks[c][s]
        place = pl.ds(starts[c], widths[c])
        arrived = (pl.ds(left, sum(size for _, size, _ in sends)), slice(None), place)
        pltpu.make_async_remote_copy(
            src_ref=gram.at[arrived], dst_ref=inbox.at[arrived],
            send_sem=send_sem, recv_sem=recv_sem.at[marks[c, s]], device_id={"rows": partners[1]},
        ).wait_recv()
        total = gram[pl.ds(0, left), :, place]
        for slot, size, _ in reversed(sends):
            total = total + inbox[pl.ds(slot, size), :, place]
        if s < len(walks[c]) - 1:
            gram[pl.ds(0, left), :, place] = total
            for copy in exchanges(c, s + 1):
                copy.start()
        else:
            gram_out[:, place] = total[0]

    def run(order):
        for code in order:
            if code < 0:
                issue(-1 - code)
            else:
                add(code // 8, code % 8)

    for z, order in enumerate(ORDERS):
        pl.when(level == z)(functools.partial(run, order))

    for j in range(len(peers)):
        weight_exchange(j).wait()
    factor = math.sqrt(row_count * rows)
    weights = jnp.concatenate([query_weight[j, 0:1, :QUERY_GROUP] for j in range(cols)], axis=1)
    owner = lax.broadcasted_iota(jnp.int32, (share, count), 0) + me * share
    lane = lax.broadcasted_iota(jnp.int32, (share, count), 1)
    weight = jnp.sum(jnp.where(owner == lane, factor * weights, 0.0), axis=1, keepdims=True)
    gram_out[...] = gram_out[...] * weight
    rest = pl.ds(1, rows - 1)
    pltpu.make_async_remote_copy(
        src_ref=gram.at[rest], dst_ref=inbox.at[rest],
        send_sem=send_sem, recv_sem=recv_sem.at[0], device_id={"rows": partners[1]},
    ).wait_send()
    rest = (pl.ds(0, 2), slice(None), pl.ds(0, width // rows * (rows - 1)))
    pltpu.make_async_remote_copy(
        src_ref=squares_inbox.at[rest], dst_ref=squares_inbox.at[rest],
        send_sem=squares_send, recv_sem=squares_recv.at[0], device_id={"rows": partners[1]},
    ).wait_send()


def kernel_shards(rows, cols, widths, groups, events, sample_mask, keep_rate):
    row_count, width = events.shape
    blocks = sample_mask.shape[1]
    bits = rows.bit_length() - 1
    count = QUERY_GROUP * cols
    share = count // rows
    steps = sum(len(path) for path, _ in PLAN)
    vmem = pl.BlockSpec(memory_space=pltpu.VMEM)
    dma = pltpu.SemaphoreType.DMA
    gram, weight = pl.pallas_call(
        functools.partial(kernel, rows, cols, widths, groups),
        out_shape=(
            jax.ShapeDtypeStruct((share, width), jnp.float32),
            jax.ShapeDtypeStruct((1, width), jnp.float32),
        ),
        in_specs=[pl.BlockSpec(memory_space=pl.ANY)] * 3,
        out_specs=(vmem, vmem),
        scratch_shapes=[
            pltpu.VMEM((row_count, width), jnp.float32),
            pltpu.VMEM((rows, share, width), jnp.float32),
            pltpu.VMEM((rows, share, width), jnp.float32),
            pltpu.VMEM((row_count, LANES), jnp.float32),
            pltpu.VMEM((cols, QUERY_GROUP, row_count), jnp.float32),
            pltpu.VMEM((1, width), jnp.float32),
            pltpu.VMEM((bits, 1, width), jnp.float32),
            pltpu.VMEM((1, width), jnp.float32),
            pltpu.VMEM((cols, SUBLANES, LANES), jnp.float32),
            pltpu.VMEM((blocks, row_count), jnp.int32),
            pltpu.SMEM((1, blocks), jnp.float32),
            pltpu.VMEM((row_count, blocks), jnp.bfloat16),
            dma((len(groups),)),
            dma((3,)),
            pltpu.SemaphoreType.REGULAR((2,)),
            dma((cols - 1,)),
            dma((cols - 1,)),
            dma((cols - 1,)),
            dma((cols - 1,)),
            dma,
            dma((steps,)),
            dma,
            dma((2 * bits,)),
        ],
        compiler_params=pltpu.CompilerParams(
            collective_id=0, has_side_effects=True, vmem_limit_bytes=48 * 2**20
        ),
    )(
        events,
        pltpu.with_memory_space_constraint(sample_mask.T, pltpu.HBM),
        pltpu.with_memory_space_constraint(keep_rate[None, :], pltpu.HBM),
    )
    return gram * weight


def solution(mesh):
    placed = (P("rows", "cols"), P("rows", "cols"), P("cols"))
    rows, cols = mesh.shape["rows"], mesh.shape["cols"]
    count = QUERY_GROUP * cols
    units = sum(size for _, size in PLAN)

    def shards(events, sample_mask, keep_rate):
        width = events.shape[1]
        fits = rows == 2 ** len(SQUARES_PATH) and count == rows * SUBLANES and width % (units * LANES) == 0 and cols == 2
        if not fits:
            return plain_shards(events, sample_mask, keep_rate)
        widths = [width // units * size for _, size in PLAN]
        sizes = [width // units * size for size in GROUPS]
        groups = [(sum(sizes[:g]), size) for g, size in enumerate(sizes)]
        return kernel_shards(rows, cols, widths, groups, events, sample_mask, keep_rate)

    return jax.shard_map(
        shards, mesh=mesh, in_specs=placed, out_specs=P("rows", "cols"), check_vma=False
    )
```

```python
import functools
import math

import jax
import jax.numpy as jnp
from jax import lax
from jax.experimental import pallas as pl
from jax.experimental.pallas import tpu as pltpu
from jax.sharding import PartitionSpec as P

QUERY_GROUP = 64
LANES = 128
SUBLANES = 8

epsilon = 1e-06

X, Y, LOW, HIGH, WIDE = 0, 1, 2, 3, 4
PLAN = (
    ((X, WIDE, Y), 4),
    ((Y, WIDE, X), 4),
    ((LOW, HIGH, X, Y), 4),
    ((LOW, Y, X, HIGH), 2),
    ((X, Y, LOW, HIGH), 4),
    ((LOW, Y, X, HIGH), 2),
    ((LOW, Y, X, HIGH), 2),
    ((Y, X, LOW, HIGH), 4),
    ((Y, X, WIDE), 4),
    ((LOW, Y, X, HIGH), 2),
    ((X, LOW, HIGH, Y), 2),
    ((X, Y, WIDE), 2),
    ((X, Y, WIDE), 2),
    ((Y, WIDE, X), 2),
    ((Y, X, WIDE), 2),
    ((X, Y, WIDE), 2),
    ((Y, X, LOW, HIGH), 2),
    ((X, Y, WIDE), 2),
    ((Y, X, WIDE), 2),
    ((X, Y, LOW, HIGH), 2),
    ((X, LOW, Y, HIGH), 4),
    ((Y, X, WIDE), 2),
    ((X, Y, WIDE), 2),
    ((LOW, Y, X, HIGH), 2),
    ((LOW, Y, X, HIGH), 2),
)
SQUARES_PATH = (X, Y, LOW, HIGH)
GROUPS = (12, 20, 16, 16)
EARLY = 3
HELD = (10, 11, 12, 13, 14, 15, 16, 17, 18, 19, 20, 21, 22, 23, 24, )
ORDERS = (
    (
        -26, -11, 0, 8, 16, -12, 24, -13, 32, 56, 200, -14, 40, -15, -16, 80, -17, -18,
        48, -19, 64, -20, -21, 88, 25, 96, -22, 33, 201, 17, -23, 57, 72, 104, -24, 41,
        120, 1, 112, 136, 81, 9, 128, 65, 34, 202, 49, -25, 58, 152, 144, 89, 184, 97,
        105, 82, 160, 26, 168, 35, 203, 18, 73, 121, 2, 192, 176, 66, 42, 137, 113, 59,
        153, 10, 204, 27, 185, 129, 83, 50, 19, 161, 90, 205, 145, 193, 106, 43, 177, 169,
        74, 154, 98, 186, 122, 162, 130, 206, 194, 138, 51, 114, 75, 146, 207, 187, 178, 163,
        170, 131, 155, 195,
    ),
    (
        -26, -11, 16, 0, 8, 24, -12, 40, -13, 32, 56, 200, -14, -15, 48, -16, 80, -17,
        -18, 72, -19, 64, -20, -21, 88, 25, 41, 96, -22, 33, 201, -23, 57, 17, -24, 104,
        120, 1, 112, 81, 136, 49, 34, 202, 9, 65, 58, 128, -25, 73, 152, 105, 184, 144,
        89, 97, 160, 26, 42, 82, 168, 35, 203, 192, 121, 66, 176, 2, 204, 18, 137, 113,
        153, 50, 10, 59, 161, 185, 83, 90, 129, 74, 193, 106, 177, 145, 19, 98, 154, 205,
        169, 27, 130, 186, 162, 122, 194, 138, 114, 206, 43, 146, 178, 207, 170, 51, 75, 155,
        187, 131, 163, 195,
    ),
    (
        -26, -11, 0, 8, 16, -12, 24, -13, 32, 56, 200, -14, 40, -15, -16, 80, -17, 48,
        -18, -19, 64, -20, -21, 88, 72, 25, 96, -22, 33, 201, -23, 57, 104, -24, 1, 41,
        120, 17, 112, 136, 9, 81, 128, 65, 34, 49, 202, -25, 152, 105, 144, 82, 89, 184,
        73, 58, 35, 97, 203, 160, 26, 168, 66, 2, 59, 176, 42, 121, 192, 18, 137, 113,
        90, 153, 10, 83, 27, 204, 129, 185, 50, 43, 161, 106, 177, 98, 145, 193, 74, 19,
        122, 205, 169, 51, 138, 186, 114, 162, 130, 154, 194, 206, 75, 146, 155, 187, 163, 178,
        131, 195, 170, 207,
    ),
    (
        -26, -11, 16, 0, 8, -12, 24, 17, -13, 32, 56, 200, -14, -15, -16, 80, -17, 40,
        -18, -19, 64, -20, -21, 88, 25, 18, -22, 33, 48, 201, 96, -23, 72, 104, -24, 57,
        1, 9, 112, 120, 81, 128, 136, 41, 34, 202, 82, 65, 35, 203, -25, 144, 58, 89,
        105, 152, 19, 168, 59, 184, 49, 66, 160, 97, 26, 73, 2, 176, 27, 121, 192, 10,
        204, 90, 98, 137, 113, 83, 129, 153, 42, 43, 185, 145, 106, 177, 161, 122, 138, 169,
        193, 114, 50, 51, 74, 154, 75, 205, 186, 130, 178, 162, 194, 206, 146, 155, 170, 131,
        187, 163, 195, 207,
    ),
)


def widen_blocks(values):
    spread = jnp.broadcast_to(values[..., None], values.shape + (128,))
    return spread.reshape(values.shape[:-1] + (values.shape[-1] * 128,))


def transposed_product(left, right):
    return lax.dot_general(
        left,
        right,
        (((0,), (0,)), ((), ())),
        precision=lax.Precision.HIGHEST,
        preferred_element_type=jnp.float32,
    )


def plain_shards(events, sample_mask, keep_rate):
    row_count, width = events.shape
    blocks = sample_mask.shape[1]
    keeping = sample_mask.astype(jnp.float32)[:, :, None]
    sampled = (events.reshape(row_count, blocks, 128) * keeping).reshape(row_count, width)
    local_squares = jnp.sum(events * events, axis=0)
    rates = widen_blocks(keep_rate)
    picked = sampled[:, :QUERY_GROUP]
    queries, query_part, query_rate = (
        lax.all_gather(picked, "cols", axis=1, tiled=True),
        lax.all_gather(local_squares[None, :QUERY_GROUP], "cols", axis=1, tiled=True),
        lax.all_gather(rates[None, :QUERY_GROUP], "cols", axis=1, tiled=True),
    )
    devices = lax.axis_size("rows")
    factor = math.sqrt(row_count * devices)
    count = queries.shape[1]
    share = count // devices
    place = lax.axis_index("rows")
    column_squares, query_squares = lax.psum((local_squares, query_part[0]), "rows")
    gram = lax.psum_scatter(
        transposed_product(queries, sampled), "rows", scatter_dimension=0, tiled=True
    )
    owned = lax.dynamic_slice_in_dim(query_squares * query_rate[0], place * share, share)
    query_weight = lax.rsqrt(owned + epsilon)
    column_weight = lax.rsqrt(column_squares * rates + epsilon)
    return factor * query_weight[:, None] * gram * column_weight[None, :]


def flipped(index, bit):
    step = 2**bit
    return index + step - 2 * step * ((index // step) % 2)


def split(values):
    high = values.astype(jnp.bfloat16)
    low = (values - high.astype(jnp.float32)).astype(jnp.bfloat16)
    return high, low


def steps_of(path, rows):
    left, found = rows, []
    for kind in path:
        if kind == WIDE:
            left //= 4
            sends = [(k * left, left, k << LOW) for k in (3, 2, 1)]
        else:
            left //= 2
            sends = [(left, left, 1 << kind)]
        found.append((left, sends))
    return found


def bits_of(path):
    return [b for kind in path for b in ((HIGH, LOW) if kind == WIDE else (kind,))]


def kernel(
    rows, cols, widths, groups,
    events_ref, mask_ref, rate_ref,
    gram_out,
    events, gram, inbox, first, queries, squares, squares_inbox, totals, query_weight, weight_row, scale,
    mask_in, rate_in, mask, load_sem, first_sem, far_sem, query_send, query_recv, weight_send, weight_recv,
    send_sem, recv_sem, squares_send, squares_recv,
):
    bits = rows.bit_length() - 1
    quad = rows // 4
    me, mine = lax.axis_index("rows"), lax.axis_index("cols")
    level = me // quad
    row_count, width = events.shape
    blocks = mask_ref.shape[0]
    share = gram.shape[1]
    count = rows * share
    starts = [sum(widths[:c]) for c in range(len(widths))]
    last = len(widths)

    heads = [
        pltpu.make_async_copy(mask_ref, mask_in, first_sem.at[0]),
        pltpu.make_async_copy(events_ref.at[:, pl.ds(0, LANES)], first, first_sem.at[1]),
        pltpu.make_async_copy(rate_ref, rate_in, first_sem.at[2]),
    ]
    for head in heads:
        head.start()
    loads = []
    for g, (start, size) in enumerate(groups):
        place = pl.ds(start, size)
        load = pltpu.make_async_copy(events_ref.at[:, place], events.at[:, place], load_sem.at[g])
        loads.append(load)
    for load in loads[:1]:
        load.start()

    partners = {1 << b: flipped(me, b) for b in range(bits)}
    partners[1 << LOW | 1 << HIGH] = flipped(partners[1 << LOW], HIGH)
    peers = [lax.rem(mine + j, cols) for j in range(1, cols)]
    barrier = pltpu.get_barrier_semaphore()
    for b in (X, Y):
        pl.semaphore_signal(barrier, inc=1, device_id={"rows": partners[1 << b]})
    for peer in peers:
        pl.semaphore_signal(barrier, inc=1, device_id={"cols": peer})

    @pl.when(level > 0)
    def _():
        pl.semaphore_signal(barrier, inc=1, device_id={"rows": me - quad})

    @pl.when(level < 3)
    def _():
        pl.semaphore_signal(barrier, inc=1, device_id={"rows": me + quad})

    for head in heads[:2]:
        head.wait()
    keeping = mask_in[...].astype(jnp.float32)
    queries[mine] = first[...].T[:QUERY_GROUP] * keeping[0:1]
    mask[...] = keeping.T.astype(jnp.bfloat16)
    pl.semaphore_wait(barrier, cols + 2 + (level * (3 - level) + 1) // 2)

    shared = []
    for j, peer in enumerate(peers):
        copy = pltpu.make_async_remote_copy(
            src_ref=queries.at[mine], dst_ref=queries.at[mine],
            send_sem=query_send.at[j], recv_sem=query_recv.at[j], device_id={"cols": peer},
        )
        copy.start()
        shared.append(copy)

    for load in loads[1:]:
        load.start()

    @pl.when((level == 1) | (level == 2))
    def _():
        pl.semaphore_signal(far_sem.at[0], inc=1, device_id={"rows": me - quad})
        pl.semaphore_signal(far_sem.at[0], inc=1, device_id={"rows": me + quad})

    own = [(me // 2**b) % 2 for b in range(bits)]
    kept_slots = {}

    def slots(path, other=None):
        order = bits_of(path)
        key = tuple(order), other is None
        if other is None and key in kept_slots:
            return kept_slots[key]
        parts = []
        for k, b in enumerate(order):
            weight = 2 ** (bits - 1 - k)
            same = own[b] * weight
            parts.append((same, weight - same) if other is None or b != HIGH else (other * weight, 0))
        half = bits // 2
        upper, lower = {}, {}
        for pick in range(2**half):
            upper[pick] = sum(parts[k][pick >> k & 1] for k in range(half))
            lower[pick] = sum(parts[half + k][pick >> k & 1] for k in range(half))
        found = []
        for d in range(rows if other is None else rows // 2):
            picks = [d >> b & 1 for b in order]
            found.append(
                upper[sum(p << k for k, p in enumerate(picks[:half]))]
                + lower[sum(p << k for k, p in enumerate(picks[half:]))]
            )
        if other is None:
            kept_slots[key] = found
        return found

    walks = [steps_of(path, rows) for path, _ in PLAN]
    marks = {}
    for c, walk in enumerate(walks):
        for s in range(len(walk)):
            marks[c, s] = len(marks)

    def exchange(c, s, k):
        slot, size, flips = walks[c][s][1][k]
        part = (pl.ds(slot, size), slice(None), pl.ds(starts[c], widths[c]))
        return pltpu.make_async_remote_copy(
            src_ref=gram.at[part], dst_ref=inbox.at[part],
            send_sem=send_sem, recv_sem=recv_sem.at[marks[c, s]], device_id={"rows": partners[flips]},
        )

    def exchanges(c, s):
        return [exchange(c, s, k) for k in range(len(walks[c][s][1]))]

    def square_range(s, sent):
        at = 0
        for k in range(s + 1):
            bit = own[SQUARES_PATH[k]]
            if k == s and sent:
                bit = 1 - bit
            at = at + bit * (width // 2 ** (k + 1))
        return pl.ds(pl.multiple_of(at, LANES), width // 2 ** (s + 1))

    def square_exchange(s):
        if s < bits:
            place = square_range(s, True)
            source, target, b = squares.at[:, place], squares_inbox.at[s, :, place], SQUARES_PATH[s]
        else:
            b = 2 * bits - 1 - s
            place = square_range(b, False)
            source, target, b = totals.at[:, place], totals.at[:, place], SQUARES_PATH[b]
        return pltpu.make_async_remote_copy(
            src_ref=source, dst_ref=target,
            send_sem=squares_send, recv_sem=squares_recv.at[s], device_id={"rows": partners[1 << b]},
        )

    def weight_exchange(j):
        return pltpu.make_async_remote_copy(
            src_ref=query_weight.at[mine], dst_ref=query_weight.at[mine],
            send_sem=weight_send.at[j], recv_sem=weight_recv.at[j], device_id={"cols": peers[j]},
        )

    def sampled(g):
        start, size = groups[g]
        loads[g].wait()
        place = pl.ds(start, size)
        values = events[:, place]
        squares[:, place] = jnp.sum(values * values, axis=0, keepdims=True)
        block_of = lax.broadcasted_iota(jnp.int32, (blocks, size), 1) // LANES + start // LANES
        spread = lax.broadcasted_iota(jnp.int32, (blocks, size), 0) == block_of
        spread = spread.astype(jnp.float32).astype(jnp.bfloat16)
        return split(values * jnp.dot(mask[...], spread, preferred_element_type=jnp.float32))

    def multiplied(rows_split, kept):
        high, low = rows_split
        lines = high.shape[0]
        both = jnp.concatenate([high, low], axis=0)
        pair = jnp.dot(both, kept[0], preferred_element_type=jnp.float32)
        rest = jnp.dot(high, kept[1], preferred_element_type=jnp.float32)
        return pair[:lines] + (pair[lines:] + rest)

    def half_send(c, whose):
        slot, size, flips = walks[c][0][1][0]
        part = size // 2
        at = slot + (whose + own[HIGH] - 2 * whose * own[HIGH]) * part
        place = (pl.ds(at, part), slice(None), pl.ds(starts[c], widths[c]))
        return pltpu.make_async_remote_copy(
            src_ref=gram.at[place], dst_ref=inbox.at[place],
            send_sem=send_sem, recv_sem=recv_sem.at[marks[c, 0]], device_id={"rows": partners[flips]},
        )

    start, size = groups[0]
    kept = sampled(0)
    for turn in range(cols):
        whose = lax.rem(mine + turn, cols)
        if turn:
            for copy in shared:
                copy.wait()
        product = multiplied(split(queries[whose]), kept)
        for c in range(EARLY):
            other = whose + own[HIGH] - 2 * whose * own[HIGH]
            chosen = slots(PLAN[c][0], other)
            for d in range(rows // cols):
                gram[chosen[d], :, pl.ds(starts[c], widths[c])] = product[
                    d * share : (d + 1) * share, starts[c] : starts[c] + widths[c]
                ]
            half_send(c, whose).start()

    everyone = split(jnp.concatenate([queries[j] for j in range(cols)], axis=0))
    for g in range(1, len(groups)):
        start, size = groups[g]
        product = multiplied(everyone, sampled(g))
        for c in range(EARLY, last):
            begin, end = max(start, starts[c]), min(start + size, starts[c] + widths[c])
            if begin < end:
                chosen = slots(PLAN[c][0])
                for d in range(rows):
                    gram[chosen[d], :, pl.ds(begin, end - begin)] = product[d * share : (d + 1) * share, begin - start : end - start]
            if begin < end == starts[c] + widths[c] and c not in HELD:
                for copy in exchanges(c, 0):
                    copy.start()

    heads[2].wait()
    pl.semaphore_wait(far_sem.at[0], 1)
    pl.semaphore_signal(far_sem.at[1], inc=1, device_id={"rows": partners[1 << LOW]})
    pl.semaphore_wait(far_sem.at[1], 1)

    def issue(c):
        if c == last:
            square_exchange(0).start()
        else:
            for copy in exchanges(c, 0):
                copy.start()

    def add_squares(s):
        square_exchange(s).wait_recv()
        if s < bits:
            place = square_range(s, False)
            value = squares[:, place] + squares_inbox[s, :, place]
            if s < bits - 1:
                squares[:, place] = value
            else:
                totals[:, place] = value
        if s < 2 * bits - 1:
            square_exchange(s + 1).start()
            return
        query_weight[mine] = jnp.broadcast_to(
            lax.rsqrt(totals[:, pl.ds(0, LANES)] * rate_in[0, 0] + epsilon), (SUBLANES, LANES)
        )
        for j in range(len(peers)):
            weight_exchange(j).start()

        def widen(b, carry):
            place = pl.ds(pl.multiple_of(b * LANES, LANES), LANES)
            weight_row[:, place] = lax.rsqrt(totals[:, place] * rate_in[0, b] + epsilon)
            return carry

        lax.fori_loop(0, blocks, widen, 0)

    def add(c, s, scaled):
        if c == last:
            add_squares(s)
            return
        left, sends = walks[c][s]
        place = pl.ds(starts[c], widths[c])
        arrived = (pl.ds(left, sum(size for _, size, _ in sends)), slice(None), place)
        pltpu.make_async_remote_copy(
            src_ref=gram.at[arrived], dst_ref=inbox.at[arrived],
            send_sem=send_sem, recv_sem=recv_sem.at[marks[c, s]], device_id={"rows": partners[1]},
        ).wait_recv()
        total = gram[pl.ds(0, left), :, place]
        for slot, size, _ in reversed(sends):
            total = total + inbox[pl.ds(slot, size), :, place]
        if s < len(walks[c]) - 1:
            gram[pl.ds(0, left), :, place] = total
            for copy in exchanges(c, s + 1):
                copy.start()
        elif scaled:
            gram_out[:, place] = total[0] * scale[:, 0:1] * weight_row[:, place]
        else:
            gram_out[:, place] = total[0]

    def weigh(waiting):
        for j in range(len(peers)):
            weight_exchange(j).wait()
        factor = math.sqrt(row_count * rows)
        weights = jnp.concatenate([query_weight[j, 0:1, :QUERY_GROUP] for j in range(cols)], axis=1)
        owner = lax.broadcasted_iota(jnp.int32, (share, count), 0) + me * share
        lane = lax.broadcasted_iota(jnp.int32, (share, count), 1)
        weight = jnp.sum(jnp.where(owner == lane, factor * weights, 0.0), axis=1, keepdims=True)
        scale[...] = jnp.broadcast_to(weight, (share, LANES))
        for c in waiting:
            place = pl.ds(starts[c], widths[c])
            gram_out[:, place] = gram_out[:, place] * weight * weight_row[:, place]

    def run(order):
        turn = max(order.index(8 * last + 2 * bits - 1) + 1, len(order) - 2)
        waiting = []
        for at, code in enumerate(order):
            if at == turn:
                weigh(waiting)
            if code < 0:
                issue(-1 - code)
                continue
            c, s = code // 8, code % 8
            add(c, s, at >= turn)
            if c < last and s == len(walks[c]) - 1:
                waiting.append(c)
        if turn == len(order):
            weigh(waiting)

    for z, order in enumerate(ORDERS):
        pl.when(level == z)(functools.partial(run, order))

    rest = pl.ds(1, rows - 1)
    pltpu.make_async_remote_copy(
        src_ref=gram.at[rest], dst_ref=inbox.at[rest],
        send_sem=send_sem, recv_sem=recv_sem.at[0], device_id={"rows": partners[1]},
    ).wait_send()
    rest = (pl.ds(0, 2), slice(None), pl.ds(0, width // rows * (rows - 1)))
    pltpu.make_async_remote_copy(
        src_ref=squares_inbox.at[rest], dst_ref=squares_inbox.at[rest],
        send_sem=squares_send, recv_sem=squares_recv.at[0], device_id={"rows": partners[1]},
    ).wait_send()


def kernel_shards(rows, cols, widths, groups, events, sample_mask, keep_rate):
    row_count, width = events.shape
    blocks = sample_mask.shape[1]
    bits = rows.bit_length() - 1
    count = QUERY_GROUP * cols
    share = count // rows
    steps = sum(len(path) for path, _ in PLAN)
    dma = pltpu.SemaphoreType.DMA
    return pl.pallas_call(
        functools.partial(kernel, rows, cols, widths, groups),
        out_shape=jax.ShapeDtypeStruct((share, width), jnp.float32),
        in_specs=[pl.BlockSpec(memory_space=pl.ANY)] * 3,
        out_specs=pl.BlockSpec(memory_space=pltpu.VMEM),
        scratch_shapes=[
            pltpu.VMEM((row_count, width), jnp.float32),
            pltpu.VMEM((rows, share, width), jnp.float32),
            pltpu.VMEM((rows, share, width), jnp.float32),
            pltpu.VMEM((row_count, LANES), jnp.float32),
            pltpu.VMEM((cols, QUERY_GROUP, row_count), jnp.float32),
            pltpu.VMEM((1, width), jnp.float32),
            pltpu.VMEM((bits, 1, width), jnp.float32),
            pltpu.VMEM((1, width), jnp.float32),
            pltpu.VMEM((cols, SUBLANES, LANES), jnp.float32),
            pltpu.VMEM((1, width), jnp.float32),
            pltpu.VMEM((share, LANES), jnp.float32),
            pltpu.VMEM((blocks, row_count), jnp.int32),
            pltpu.SMEM((1, blocks), jnp.float32),
            pltpu.VMEM((row_count, blocks), jnp.bfloat16),
            dma((len(groups),)),
            dma((3,)),
            pltpu.SemaphoreType.REGULAR((2,)),
            dma((cols - 1,)),
            dma((cols - 1,)),
            dma((cols - 1,)),
            dma((cols - 1,)),
            dma,
            dma((steps,)),
            dma,
            dma((2 * bits,)),
        ],
        compiler_params=pltpu.CompilerParams(
            collective_id=0, has_side_effects=True, vmem_limit_bytes=48 * 2**20
        ),
    )(
        events,
        pltpu.with_memory_space_constraint(sample_mask.T, pltpu.HBM),
        pltpu.with_memory_space_constraint(keep_rate[None, :], pltpu.HBM),
    )


def solution(mesh):
    placed = (P("rows", "cols"), P("rows", "cols"), P("cols"))
    rows, cols = mesh.shape["rows"], mesh.shape["cols"]
    count = QUERY_GROUP * cols
    units = sum(size for _, size in PLAN)

    def shards(events, sample_mask, keep_rate):
        width = events.shape[1]
        fits = rows == 2 ** len(SQUARES_PATH) and count == rows * SUBLANES and width % (units * LANES) == 0 and cols == 2
        if not fits:
            return plain_shards(events, sample_mask, keep_rate)
        widths = [width // units * size for _, size in PLAN]
        sizes = [width // units * size for size in GROUPS]
        groups = [(sum(sizes[:g]), size) for g, size in enumerate(sizes)]
        return kernel_shards(rows, cols, widths, groups, events, sample_mask, keep_rate)

    return jax.shard_map(
        shards, mesh=mesh, in_specs=placed, out_specs=P("rows", "cols"), check_vma=False
    )
```
